16 devices in a mesh: rep: 1, dp: 16 (over x, y, z, core).
Axes of the slice: x: 2, y: 2, z: 2, core: 2. Of those that a mesh axis runs over, the one named last changes fastest.
Arguments:
- x: bfloat16 [16, 2048, 1536], P(('rep', 'dp'))
- dy: bfloat16 [16, 2048, 1536], P(('rep', 'dp'))
- w_gate: bfloat16 [2, 1536, 4096], P(None, 'dp')
- w_up: bfloat16 [2, 1536, 4096], P(None, 'dp')
- w_down: bfloat16 [2, 4096, 1536], P(None, 'dp')
- m_w_gate: float32 [2, 1536, 4096], P(None, 'dp')
- m_w_up: float32 [2, 1536, 4096], P(None, 'dp')
- m_w_down: float32 [2, 4096, 1536], P(None, 'dp')
- v_w_gate: float32 [2, 1536, 4096], P(None, 'dp')
- v_w_up: float32 [2, 1536, 4096], P(None, 'dp')
- v_w_down: float32 [2, 4096, 1536], P(None, 'dp')
Outputs:
- output 1: bfloat16 [2, 1536, 4096], P('rep', 'dp')
- output 2: bfloat16 [2, 1536, 4096], P('rep', 'dp')
- output 3: bfloat16 [2, 4096, 1536], P('rep', 'dp')
- output 4: float32 [2, 1536, 4096], P('rep', 'dp')
- output 5: float32 [2, 1536, 4096], P('rep', 'dp')
- output 6: float32 [2, 4096, 1536], P('rep', 'dp')
- output 7: float32 [2, 1536, 4096], P('rep', 'dp')
- output 8: float32 [2, 1536, 4096], P('rep', 'dp')
- output 9: float32 [2, 4096, 1536], P('rep', 'dp')
All inputs are finite; a program needn't handle non-finite values.
Results may differ from the reference program's by a relative error of at most 0.022.
Values are sent between devices in bfloat16 or wider.
A program may use at most 2 GiB of HBM per device.

```python
import jax
import jax.numpy as jnp
from jax import lax

SEQUENCES = 16
TOKENS = 2048
D = 1536
FF = 4096
LAYERS = 2
NAMES = ("w_gate", "w_up", "w_down")
SHAPES = {"w_gate": (LAYERS, D, FF), "w_up": (LAYERS, D, FF), "w_down": (LAYERS, FF, D)}


def bump(key, n, height):
    away = (jnp.arange(n, dtype=jnp.int32) - jax.random.randint(key, (), 0, n, jnp.int32)) % n
    return jnp.where(away < n // 8, height, 1.0)


def together(key, own, strength):
    shared = jax.random.normal(key, own.shape[1:], jnp.float32)
    return (own + strength * shared) * lax.rsqrt(1 + strength * strength)


def setup_inputs(seed: int = 0, part: int = 0) -> dict:
    kx, kdy, ka, kb, kz, kf, kh, kl, *keys = jax.random.split(jax.random.key(seed), 8 + 3 * len(NAMES))
    kx, kdy, ka, kb = (jax.random.fold_in(k, part) for k in (kx, kdy, ka, kb))
    kw, km, kv = (keys[i::3] for i in range(3))
    shape = (SEQUENCES, TOKENS, D)
    much_x, much_dy = jax.random.uniform(kz, (2,), jnp.float32, 0.0, 1.0)
    loud = 2.0 ** jax.random.uniform(jax.random.fold_in(kz, 1), (), jnp.float32, -1.0, 2.0)
    layers = 2.0 ** jax.random.uniform(kl, (LAYERS, 1, 1), jnp.float32, -1.0, 1.0)
    x = together(ka, jax.random.normal(kx, shape, jnp.float32), much_x) * bump(kf, D, 4.0)
    dy = together(kb, jax.random.normal(kdy, shape, jnp.float32), much_dy)
    drawn = {"x": x.astype(jnp.bfloat16), "dy": (loud * dy * (SEQUENCES * TOKENS) ** -0.5).astype(jnp.bfloat16)}
    for key, name in zip(kw, NAMES, strict=True):
        w = jax.random.normal(key, SHAPES[name], jnp.float32) * SHAPES[name][1] ** -0.5
        drawn[name] = (w * {"w_gate": 1.0, "w_up": bump(kh, FF, 4.0), "w_down": layers}[name]).astype(jnp.bfloat16)
    for key, name in zip(km, NAMES, strict=True):
        drawn[f"m_{name}"] = 0.1 * jax.random.normal(key, SHAPES[name], jnp.float32)
    for key, name in zip(kv, NAMES, strict=True):
        drawn[f"v_{name}"] = jax.random.uniform(key, SHAPES[name], jnp.float32, 0.005, 0.015)
    return drawn


def matmul(a, w):
    return jnp.dot(a, w, preferred_element_type=jnp.float32).astype(jnp.bfloat16)


def normed(h):
    wide = h.astype(jnp.float32)
    scale = lax.rsqrt(jnp.mean(wide**2, -1, keepdims=True) + 1e-6)
    return (wide * scale).astype(jnp.bfloat16)


def layer(h, w):
    a = normed(h)
    gate = jnp.dot(a, w["w_gate"], preferred_element_type=jnp.float32)
    up = jnp.dot(a, w["w_up"], preferred_element_type=jnp.float32)
    return h + matmul((jax.nn.silu(gate) * up).astype(jnp.bfloat16), w["w_down"])


def adamw(w, m, v, g):
    m = 0.9 * m + 0.1 * g
    v = 0.95 * v + 0.05 * g * g
    step = m * lax.rsqrt(v + 1e-8) + 0.1 * w
    return (w - 0.02 * step).astype(jnp.bfloat16), m, v


def clipped(gradients, sum_of_squares, count):
    factor = jnp.minimum(1.0, 0.5 * lax.rsqrt(sum_of_squares / count + 1e-30))
    return [g * factor for g in gradients]


def stack(weights, h):
    return lax.scan(lambda h, w: (layer(h, w), None), h, weights)[0]


def reference(x, dy, w_gate, w_up, w_down, m_w_gate, m_w_up, m_w_down, v_w_gate, v_w_up, v_w_down):
    weights = dict(zip(NAMES, (w_gate, w_up, w_down), strict=True))

    def take(so_far, sequence):
        h, by_y = sequence
        _, back = jax.vjp(lambda w: stack(w, h), weights)
        return jax.tree.map(lambda total, term: total + term.astype(jnp.float32), so_far, back(by_y)[0]), None

    none_yet = {name: jnp.zeros(w.shape, jnp.float32) for name, w in weights.items()}
    by_weights, _ = lax.scan(take, none_yet, (x, dy))
    gradients = [by_weights[name].astype(jnp.bfloat16).astype(jnp.float32) for name in NAMES]
    gradients = clipped(gradients, sum(jnp.sum(g * g) for g in gradients), sum(g.size for g in gradients))
    new = [
        adamw(w.astype(jnp.float32), m, v, g)
        for w, m, v, g in zip((w_gate, w_up, w_down), (m_w_gate, m_w_up, m_w_down), (v_w_gate, v_w_up, v_w_down), gradients, strict=True)
    ]
    return tuple(one[which] for which in range(3) for one in new)
```

```python
import functools

import jax
import jax.numpy as jnp
from jax import lax
from jax.experimental import pallas as pl
from jax.experimental.pallas import tpu as pltpu
from jax.sharding import PartitionSpec as P

NAMES = ("w_gate", "w_up", "w_down")
BF, F32 = jnp.bfloat16, jnp.float32
MESH = pl.DeviceIdType.MESH
TN = (((0,), (0,)), ((), ()))
NT = (((1,), (1,)), ((), ()))
M, D, F = 2048, 1536, 4096
UNITS = 48
OWN, IN = 10, 6
LAST = 5


def dot(a, b, dims):
    return lax.dot_general(a, b, dims, preferred_element_type=F32)


def matmul(a, w):
    return jnp.dot(a, w, preferred_element_type=F32).astype(BF)


def normed(h):
    wide = h.astype(F32)
    scale = lax.rsqrt(jnp.mean(wide**2, -1, keepdims=True) + 1e-6)
    return (wide * scale).astype(BF)


def adamw(w, m, v, g):
    m = 0.9 * m + 0.1 * g
    v = 0.95 * v + 0.05 * g * g
    step = m * lax.rsqrt(v + 1e-8) + 0.1 * w
    return (w - 0.02 * step).astype(BF), m, v


class Scatter:
    def __init__(self, own, r0, ra, rb, rc, sa, sb, sc, out, squares, sems, free, g_hbm):
        self.own, self.r0, self.ra, self.rb, self.rc = own, r0, ra, rb, rc
        self.sa, self.sb, self.sc, self.out, self.squares = sa, sb, sc, out, squares
        self.sems, self.free, self.g_hbm = sems, free, g_hbm
        me = lax.axis_index("dp")
        self.core, self.chip = me % 2, me // 2
        self.bits = ((me // 8) % 2, (me // 4) % 2, (me // 2) % 2)
        self.weights = (4, 2, 1)
        self.partner = me + 1 - 2 * self.core
        self.near = tuple(me + 2 * w * (1 - 2 * b) for b, w in zip(self.bits, self.weights, strict=True))

    def copy(self, phase, src, dst, slot, color, device):
        send, recv = self.sems[phase]
        at = (slot,) if color is None else (slot, color)
        return pltpu.make_async_remote_copy(
            src_ref=src, dst_ref=dst, send_sem=send.at[at], recv_sem=recv.at[at], device_id={"dp": device}, device_id_type=MESH
        )

    def copy_0(self, u):
        slot = lax.rem(u, IN)
        return self.copy(0, self.own.at[lax.rem(u, OWN), 1 - self.core], self.r0.at[slot], slot, None, self.partner)

    def copy_a(self, u, k):
        slot = lax.rem(u, IN)
        return self.copy(1, self.sa.at[slot, k], self.ra.at[slot, k], slot, k, self.near[k])

    def copy_b(self, u, k):
        slot = lax.rem(u, IN)
        return self.copy(2, self.sb.at[slot, k], self.rb.at[slot, k], slot, k, self.near[(k + 1) % 3])

    def copy_c(self, u, k):
        slot = lax.rem(u, IN)
        return self.copy(3, self.sc.at[slot, k], self.rc.at[slot, k], slot, k, self.near[(k + 2) % 3])

    def write(self, u):
        slot = lax.rem(u, IN)
        return pltpu.make_async_copy(self.out.at[slot], self.g_hbm.at[u], self.sems[4].at[slot])

    def index(self, k, a, b, c):
        return a * self.weights[k] + b * self.weights[(k + 1) % 3] + c * self.weights[(k + 2) % 3]

    def two(self, u, k, index):
        own = self.own[lax.rem(u, OWN), self.core, index, k].astype(F32)
        return own + self.r0[lax.rem(u, IN), index, k].astype(F32)

    def phase_0(self, u):
        @pl.when(u >= IN)
        def _():
            pl.semaphore_wait(self.free.at[3], 1)

        self.copy_0(u).start()

    def phase_a(self, u):
        @pl.when(u >= IN)
        def _():
            for axis in range(3):
                pl.semaphore_wait(self.free.at[axis], 1)

        self.copy_0(u).wait_recv()
        slot = lax.rem(u, IN)
        for k in range(3):
            away = 1 - self.bits[k]
            for b in range(2):
                for c in range(2):
                    self.sa[slot, k, 2 * b + c] = self.two(u, k, self.index(k, away, b, c)).astype(BF)
            self.copy_a(u, k).start()

    def phase_b(self, u):
        slot = lax.rem(u, IN)
        for k in range(3):
            here, away = self.bits[k], 1 - self.bits[(k + 1) % 3]
            self.copy_a(u, k).wait_recv()
            for c in range(2):
                total = self.two(u, k, self.index(k, here, away, c)) + self.ra[slot, k, 2 * away + c].astype(F32)
                self.sb[slot, k, c] = total.astype(BF)
            self.copy_b(u, k).start()

    def phase_c(self, u):
        slot = lax.rem(u, IN)
        for k in range(3):
            a, b, away = self.bits[k], self.bits[(k + 1) % 3], 1 - self.bits[(k + 2) % 3]
            self.copy_b(u, k).wait_recv()
            total = self.two(u, k, self.index(k, a, b, away)) + self.ra[slot, k, 2 * b + away].astype(F32)
            self.sc[slot, k] = (total + self.rb[slot, k, away].astype(F32)).astype(BF)
            self.copy_c(u, k).start()

    def phase_d(self, u):
        slot = lax.rem(u, IN)

        @pl.when(u >= IN)
        def _():
            self.write(u - IN).wait()

        for k in range(3):
            b, c = self.bits[(k + 1) % 3], self.bits[(k + 2) % 3]
            self.copy_c(u, k).wait_recv()
            total = self.two(u, k, self.chip) + self.ra[slot, k, 2 * b + c].astype(F32)
            total = total + self.rb[slot, k, c].astype(F32) + self.rc[slot, k].astype(F32)
            rounded = total.astype(BF)
            self.out[slot, pl.ds(32 * k, 32), :] = rounded
            wide = rounded.astype(F32)
            square = wide * wide
            self.squares[...] += square[0:8] + square[8:16] + square[16:24] + square[24:32]
        self.write(u).start()
        self.copy_0(u).wait_send()
        for k in range(3):
            self.copy_a(u, k).wait_send()
            self.copy_b(u, k).wait_send()
            self.copy_c(u, k).wait_send()

        @pl.when(u + IN < UNITS)
        def _():
            pl.semaphore_signal(self.free.at[3], inc=1, device_id={"dp": self.partner}, device_id_type=MESH)
            for axis in range(3):
                pl.semaphore_signal(self.free.at[axis], inc=1, device_id={"dp": self.near[axis]}, device_id_type=MESH)

    def tick(self, q, low, high):
        for lag, phase in ((LAST, self.phase_d), (4, self.phase_c), (3, self.phase_b), (1, self.phase_a), (0, self.phase_0)):
            u = q - lag

            @pl.when((u >= low) & (u < high))
            def _(phase=phase, u=u):
                phase(u)


class Plan:
    def __init__(self):
        self.first, self.low, self.made, self.log = LAST, 0, 0, []

    def stage(self, steps, per, of, units_after):
        ticks = [j // of * per + j % of for j in range(steps) if j % of < per]
        at = [j for j in range(steps) if j % of < per]
        stage = (self.first, self.low, self.made)
        for j in range(steps):
            if j in at:
                self.log.append((self.first + ticks[at.index(j)], self.low, self.made + units_after(j)))
            for u in range(self.made + units_after(j), self.made + units_after(j + 1)):
                assert u - OWN < self.low or u - OWN <= self.log[-1][0] - LAST, u
        self.first += len(ticks)
        self.made += units_after(steps)
        return stage

    def restart(self, idle):
        assert self.first - LAST >= self.made, (self.first, self.made)
        self.first, self.low = self.made - idle, self.made

    def check(self):
        seen = {}
        for q, low, high in self.log:
            for name, lag in (("d", LAST), ("c", 4), ("b", 3), ("a", 1), ("0", 0)):
                u = q - lag
                if low <= u < high:
                    seen.setdefault(u, []).append(name)
        assert all(seen.get(u) == ["0", "a", "b", "c", "d"] for u in range(UNITS)), seen


def backward_kernel(
    dy, act1, g1, u1, a1, h1, wd1, wg1, wu1, act0, g0, u0, a0, wd0,
    dg1, du1, dg0, du0, g_hbm, total_ref,
    x1, own, r0, ra, rb, rc, sa, sb, sc, out, squares, sums, sum_all,
    s0s, s0r, sas, sar, sbs, sbr, scs, scr, out_sem, free, sum_send, sum_recv, load_sem, act_sem,
):
    me = lax.axis_index("dp")
    barrier = pltpu.get_barrier_semaphore()
    for other in range(1, 16):
        pl.semaphore_signal(barrier, inc=1, device_id={"dp": (me + other) % 16}, device_id_type=MESH)
    pl.semaphore_wait(barrier, 15)

    sems = ((s0s, s0r), (sas, sar), (sbs, sbr), (scs, scr), out_sem)
    scatter = Scatter(own, r0, ra, rb, rc, sa, sb, sc, out, squares, sems, free, g_hbm)
    plan = Plan()
    squares[...] = jnp.zeros_like(squares)
    load = pltpu.make_async_copy(dy, x1, load_sem.at[0])
    load.start()

    def down_gradient(act, made, stage, ready):
        def body(held):
            def block(f):
                return pltpu.make_async_copy(act.at[:, pl.ds(pl.multiple_of(f * 512, 512), 512)], held.at[f], act_sem.at[f])

            for f in range(8):
                block(f).start()
            ready()

            def step(t, carry):
                columns, f = t // 8, lax.rem(t, 8)

                @pl.when(t < 8)
                def _():
                    block(f).wait()

                @pl.when(lax.rem(t, 5) == 0)
                def _():
                    scatter.tick(stage[0] + t // 5, stage[1], stage[2] + 2 * columns)

                tile = dot(held[f], x1[:, pl.ds(pl.multiple_of(columns * 384, 128), 384)], TN).astype(BF)
                for half in range(2):
                    slot = lax.rem(made + 2 * columns + half, OWN)
                    for core in range(2):
                        for k in range(3):
                            for q in range(4):
                                row = 256 * core + 128 * half + 32 * q
                                own[slot, core, f, k, :, 128 * q : 128 * q + 128] = tile[row : row + 32, 128 * k : 128 * k + 128]
                return carry

            lax.fori_loop(0, 32, step, 0)

        pl.run_scoped(body, pltpu.VMEM((8, M, 512), BF))

    def hidden(wd, g, u, dg, du, stage):
        def step(w_ref, g_ref, u_ref, dg_ref, du_ref):
            f, half = pl.program_id(0), pl.program_id(1)

            @pl.when(half == 0)
            def _():
                scatter.tick(stage[0] + f, stage[1], stage[2])

            for s in range(4):
                rows = pl.ds(256 * s, 256)
                by = dot(x1[pl.ds(pl.multiple_of(half * 1024, 1024) + 256 * s, 256), :], w_ref[...], NT).astype(BF).astype(F32)
                gate, up = g_ref[rows, :], u_ref[rows, :]
                sigmoid = lax.logistic(gate)
                silu = gate * sigmoid
                du_ref[rows, :] = (by * silu).astype(BF)
                dg_ref[rows, :] = (by * up * (sigmoid + silu * (1.0 - sigmoid))).astype(BF)

        tile = pl.BlockSpec((1024, 512), lambda f, half: (half, f))
        pltpu.emit_pipeline(
            step, grid=(8, 2), in_specs=[pl.BlockSpec((512, D), lambda f, half: (f, 0)), tile, tile], out_specs=[tile, tile]
        )(wd, g, u, dg, du)

    def wide_gradient(x2, by, made, stage, per):
        def step(by_ref):
            j = pl.program_id(0)

            @pl.when(lax.rem(j, 4) < per)
            def _():
                scatter.tick(stage[0] + j // 4 * per + lax.rem(j, 4), stage[1], stage[2] + j)

            slot = lax.rem(made + j, OWN)
            for b in range(4):
                tile = dot(x2[:, 384 * b : 384 * b + 384], by_ref[...], TN).astype(BF)
                for s in range(4):
                    for k in range(3):
                        row = 96 * s + 32 * k
                        own[slot, s % 2, 2 * b + s // 2, k, :, :] = tile[row : row + 32, :]

        pltpu.emit_pipeline(step, grid=(8,), in_specs=[pl.BlockSpec((M, 512), lambda j: (0, j))], out_specs=[])(by)

    def states(stage):
        def body(da, held):
            def step(dg_ref, du_ref, wg_ref, wu_ref):
                m, n = pl.program_id(0), pl.program_id(1)
                rows = pl.ds(pl.multiple_of(m * 512, 512), 512)
                take = pltpu.make_async_copy(h1.at[rows], held, load_sem.at[2])

                @pl.when(n == 0)
                def _():
                    take.start()

                @pl.when(lax.rem(n, 2) == 0)
                def _():
                    scatter.tick(stage[0] + 3 * m + n // 2, stage[1], stage[2])

                by_gate = dot(dg_ref[...], wg_ref[...], NT).astype(BF).astype(F32)
                by_up = dot(du_ref[...], wu_ref[...], NT).astype(BF).astype(F32)
                da[n] = (by_gate + by_up).astype(BF)

                @pl.when(n == 5)
                def _():
                    take.wait()

                    def some(i, carry):
                        at = pl.ds(pl.multiple_of(i * 32, 32), 32)
                        wide = held[at, :].astype(F32)
                        scale = lax.rsqrt(jnp.mean(wide * wide, -1, keepdims=True) + 1e-6)
                        by = jnp.concatenate([da[n, at, :] for n in range(6)], axis=-1).astype(F32)
                        inner = jnp.sum(by * wide, -1, keepdims=True)
                        back = (by * scale - wide * (inner * scale * scale * scale * (1.0 / D))).astype(BF)
                        at_all = pl.ds(pl.multiple_of(m * 512 + i * 32, 32), 32)
                        x1[at_all, :] = (x1[at_all, :].astype(F32) + back.astype(F32)).astype(BF)
                        return carry

                    lax.fori_loop(0, 16, some, 0)

            tile = pl.BlockSpec((512, F), lambda m, n: (m, 0))
            rows = pl.BlockSpec((256, F), lambda m, n: (n, 0))
            pltpu.emit_pipeline(step, grid=(4, 6), in_specs=[tile, tile, rows, rows], out_specs=[])(dg1, du1, wg1, wu1)

        pl.run_scoped(body, pltpu.VMEM((6, 512, 256), BF), pltpu.VMEM((512, D), BF))

    def later(x2):
        take = pltpu.make_async_copy(a1, x2, load_sem.at[1])
        take.start()
        plan.restart(2)
        stage = plan.stage(32, 1, 5, lambda t: 2 * (t // 8))
        down_gradient(act1, 0, stage, load.wait)
        stage = plan.stage(8, 1, 1, lambda j: 0)
        hidden(wd1, g1, u1, dg1, du1, stage)
        plan.restart(1)
        take.wait()
        stage = plan.stage(8, 3, 4, lambda j: j)
        wide_gradient(x2, dg1, 8, stage, 3)
        stage = plan.stage(8, 3, 4, lambda j: j)
        wide_gradient(x2, du1, 16, stage, 3)

    def sooner(x2):
        take = pltpu.make_async_copy(a0, x2, load_sem.at[1])
        take.start()
        plan.restart(2)
        stage = plan.stage(32, 1, 5, lambda t: 2 * (t // 8))
        down_gradient(act0, 24, stage, lambda: None)
        stage = plan.stage(8, 1, 1, lambda j: 0)
        hidden(wd0, g0, u0, dg0, du0, stage)
        plan.restart(1)
        take.wait()
        stage = plan.stage(8, 4, 4, lambda j: j)
        wide_gradient(x2, dg0, 32, stage, 4)
        stage = plan.stage(8, 4, 4, lambda j: j)
        wide_gradient(x2, du0, 40, stage, 4)

    pl.run_scoped(later, pltpu.VMEM((M, D), BF))
    stage = plan.stage(12, 1, 1, lambda j: 0)
    states(stage)
    pl.run_scoped(sooner, pltpu.VMEM((M, D), BF))
    left = UNITS + LAST - plan.first
    first, low, _ = plan.stage(left, 1, 1, lambda j: 0)
    plan.check()

    def rest(t, carry):
        scatter.tick(first + t, low, UNITS)
        return carry

    lax.fori_loop(0, left, rest, 0)
    for u in range(UNITS - IN, UNITS):
        scatter.write(u).wait()

    mine = jnp.sum(squares[...], axis=(0, 1), keepdims=True)
    sums[...] = jnp.broadcast_to(mine, sums.shape)

    def tell(to, of):
        return pltpu.make_async_remote_copy(
            src_ref=sums, dst_ref=sum_all.at[of], send_sem=sum_send.at[to], recv_sem=sum_recv.at[of], device_id={"dp": to}, device_id_type=MESH
        )

    for other in range(1, 16):
        tell((me + other) % 16, me).start()
    for other in range(1, 16):
        tell((me + other) % 16, (me + other) % 16).wait_recv()
    for other in range(1, 16):
        tell((me + other) % 16, me).wait_send()
    sum_all[me] = sums[...]
    total = sum_all[0]
    for i in range(1, 16):
        total = total + sum_all[i]
    total_ref[...] = total


def backward(*args):
    any_spec = pl.BlockSpec(memory_space=pl.ANY)
    shape = jax.ShapeDtypeStruct
    piece = (3, 32, 512)
    dma = pltpu.SemaphoreType.DMA
    outs = pl.pallas_call(
        backward_kernel,
        out_shape=[shape((M, F), BF)] * 4 + [shape((UNITS, 96, 512), BF), shape((8, 128), F32)],
        in_specs=[any_spec] * 14,
        out_specs=[any_spec] * 5 + [pl.BlockSpec(memory_space=pltpu.VMEM)],
        scratch_shapes=[
            pltpu.VMEM((M, D), BF),
            pltpu.VMEM((OWN, 2, 8, *piece), BF),
            pltpu.VMEM((IN, 8, *piece), BF),
            pltpu.VMEM((IN, 3, 4, 32, 512), BF),
            pltpu.VMEM((IN, 3, 2, 32, 512), BF),
            pltpu.VMEM((IN, *piece), BF),
            pltpu.VMEM((IN, 3, 4, 32, 512), BF),
            pltpu.VMEM((IN, 3, 2, 32, 512), BF),
            pltpu.VMEM((IN, *piece), BF),
            pltpu.VMEM((IN, 96, 512), BF),
            pltpu.VMEM((8, 512), F32),
            pltpu.VMEM((8, 128), F32),
            pltpu.VMEM((16, 8, 128), F32),
            dma((IN,)), dma((IN,)),
            dma((IN, 3)), dma((IN, 3)), dma((IN, 3)), dma((IN, 3)), dma((IN, 3)), dma((IN, 3)),
            dma((IN,)),
            pltpu.SemaphoreType.REGULAR((4,)),
            dma((16,)), dma((16,)), dma((3,)), dma((8,)),
        ],
        compiler_params=pltpu.CompilerParams(collective_id=0, has_side_effects=True, vmem_limit_bytes=67_000_000),
        cost_estimate=pl.CostEstimate(flops=10 * 2 * M * D * F, bytes_accessed=600_000_000, transcendentals=0),
        name="backward",
    )(*args)
    return outs[4], outs[5]


def solution(mesh):
    def fetched(weights, number):
        return {name: lax.all_gather(w[number], "dp", axis=0, tiled=True) for name, w in zip(NAMES, weights, strict=True)}

    def step(x, dy, *arrays):
        weights, m, v = (arrays[i : i + 3] for i in (0, 3, 6))
        h, kept = x[0], []
        for number in range(2):
            w = fetched(weights, number)
            a = normed(h)
            gate = jnp.dot(a, w["w_gate"], preferred_element_type=F32)
            up = jnp.dot(a, w["w_up"], preferred_element_type=F32)
            act = (jax.nn.silu(gate) * up).astype(BF)
            kept.append((h, a, gate, up, act, w))
            h = h + matmul(act, w["w_down"])
        (_, a0, g0, u0, act0, w0), (h1, a1, g1, u1, act1, w1) = kept
        units, total = backward(
            dy[0], act1, g1, u1, a1, h1, w1["w_down"], w1["w_gate"], w1["w_up"], act0, g0, u0, a0, w0["w_down"]
        )
        count = 16 * sum(w.size for w in weights)
        factor = jnp.minimum(1.0, 0.5 * lax.rsqrt(total[0, 0] / count + 1e-30))

        def wide(first):
            return units[first : first + 8].transpose(1, 0, 2).reshape(96, F)

        def down(first):
            return units[first : first + 8].reshape(4, 2, 3, 32, 4, 128).transpose(1, 4, 3, 0, 2, 5).reshape(256, D)

        gradients = [
            jnp.stack([wide(32), wide(8)]),
            jnp.stack([wide(40), wide(16)]),
            jnp.stack([down(24), down(0)]),
        ]
        gradients = [g.astype(F32) * factor for g in gradients]
        new = [adamw(w.astype(F32), m, v, g) for w, m, v, g in zip(weights, m, v, gradients, strict=True)]
        return tuple(one[which] for which in range(3) for one in new)

    states, cut = P(("rep", "dp"), None, None), P(None, "dp", None)
    return jax.shard_map(
        step,
        mesh=mesh,
        in_specs=(states, states) + (cut,) * 9,
        out_specs=(P("rep", "dp", None),) * 9,
        check_vma=False,
    )
```

```python
import functools

import jax
import jax.numpy as jnp
from jax import lax
from jax.experimental import pallas as pl
from jax.experimental.pallas import tpu as pltpu
from jax.sharding import PartitionSpec as P

NAMES = ("w_gate", "w_up", "w_down")
BF, F32 = jnp.bfloat16, jnp.float32
MESH = pl.DeviceIdType.MESH
TN = (((0,), (0,)), ((), ()))
NT = (((1,), (1,)), ((), ()))
M, D, F = 2048, 1536, 4096
BLOCK, HALF, QUARTER = 512, 256, 128
PIECE, FEW, TALL = 32, 96, 256
COLORS, CORES, LAYERS, ROWS, DEVICES = 3, 2, 2, 64, 16
WIDTH, FOURTH, TILE = 2 * BLOCK, D // 4, (8, 128)
VMEM = 67_000_000
WEIGHTS = (4, 2, 1)
BOTH = range(CORES)
SPREAD, ZEROS = (CORES,) * 4, (0,) * 5
UNITS = 48
OWN, IN = 8, 6
GATHERS, SLOTS = 38, 10
WIDE, DOWN = ("wide",), ("down",)
HURRY = 34
LAST = 5
LAGS = (LAST, 4, 3, 1, 0)


def span(i, size):
    return pl.ds(pl.multiple_of(i * size, size), size)


def loop(first, last, do):
    def step(i, carry):
        do(i)
        return carry

    lax.fori_loop(first, last, step, 0)


def ids(n):
    return tuple(pl.program_id(i) for i in range(n))


def along(reduce, a):
    return reduce(a, -1, keepdims=True)


def bits_of(chip):
    return tuple(chip // w % 2 for w in WEIGHTS)


def place():
    me = lax.axis_index("dp")
    chip = me // CORES
    bits = bits_of(chip)
    near = tuple(me + CORES * w * (1 - 2 * b) for b, w in zip(bits, WEIGHTS))
    return me % CORES, chip, bits, me + 1 - 2 * (me % CORES), near


def dot(a, b, dims):
    return lax.dot_general(a, b, dims, preferred_element_type=F32)


def normed(h):
    wide = h.astype(F32)
    scale = lax.rsqrt(along(jnp.mean, wide * wide) + 1e-6)
    return (wide * scale).astype(BF)


def adamw(w, m, v, g):
    m = 0.9 * m + 0.1 * g
    v = 0.95 * v + 0.05 * g * g
    step = m * lax.rsqrt(v + 1e-8) + 0.1 * w
    return (w - 0.02 * step).astype(BF), m, v


class Scatter:
    def __init__(self, own, r0, ra, rb, rc, sa, sb, sc, out, squares, sems, free, g_hbm):
        self.own, self.r0, self.ra, self.rb, self.rc = own, r0, ra, rb, rc
        self.sa, self.sb, self.sc, self.out, self.squares = sa, sb, sc, out, squares
        self.sems, self.free, self.g_hbm = sems, free, g_hbm
        self.core, self.chip, self.bits, self.partner, self.near = place()

    def copy(self, phase, src, dst, slot, color, device):
        send, recv = self.sems[phase]
        at = (slot,) if color is None else (slot, color)
        return pltpu.make_async_remote_copy(
            src_ref=src, dst_ref=dst, send_sem=send.at[at], recv_sem=recv.at[at], device_id={"dp": device}, device_id_type=MESH
        )

    def copy_0(self, u):
        slot = lax.rem(u, IN)
        return self.copy(0, self.own.at[lax.rem(u, OWN), 1 - self.core], self.r0.at[slot], slot, None, self.partner)

    def copy_a(self, u, k):
        slot = lax.rem(u, IN)
        return self.copy(1, self.sa.at[slot, k], self.ra.at[slot, k], slot, k, self.near[k])

    def copy_b(self, u, k):
        slot = lax.rem(u, IN)
        return self.copy(2, self.sb.at[slot, k], self.rb.at[slot, k], slot, k, self.near[(k + 1) % COLORS])

    def copy_c(self, u, k):
        slot = lax.rem(u, IN)
        return self.copy(3, self.sc.at[slot, k], self.rc.at[slot, k], slot, k, self.near[(k + 2) % COLORS])

    def write(self, u):
        slot = lax.rem(u, IN)
        return pltpu.make_async_copy(self.out.at[slot], self.g_hbm.at[u], self.sems[4].at[slot])

    def index(self, k, a, b, c):
        return a * WEIGHTS[k] + b * WEIGHTS[(k + 1) % COLORS] + c * WEIGHTS[(k + 2) % COLORS]

    def two(self, u, k, index):
        own = self.own[lax.rem(u, OWN), self.core, index, k].astype(F32)
        return own + self.r0[lax.rem(u, IN), index, k].astype(F32)

    def phase_0(self, u):
        @pl.when(u >= IN)
        def _():
            pl.semaphore_wait(self.free.at[3], 1)

        self.copy_0(u).start()

    def phase_a(self, u):
        @pl.when(u >= IN)
        def _():
            for axis in range(COLORS):
                pl.semaphore_wait(self.free.at[axis], 1)

        self.copy_0(u).wait_recv()
        slot = lax.rem(u, IN)
        for k in range(COLORS):
            away = 1 - self.bits[k]
            for b in BOTH:
                for c in BOTH:
                    self.sa[slot, k, 2 * b + c] = self.two(u, k, self.index(k, away, b, c)).astype(BF)
            self.copy_a(u, k).start()

    def phase_b(self, u):
        slot = lax.rem(u, IN)
        for k in range(COLORS):
            here, away = self.bits[k], 1 - self.bits[(k + 1) % COLORS]
            self.copy_a(u, k).wait_recv()
            for c in BOTH:
                total = self.two(u, k, self.index(k, here, away, c)) + self.ra[slot, k, 2 * away + c].astype(F32)
                self.sb[slot, k, c] = total.astype(BF)
            self.copy_b(u, k).start()

    def phase_c(self, u):
        slot = lax.rem(u, IN)
        for k in range(COLORS):
            a, b, away = self.bits[k], self.bits[(k + 1) % COLORS], 1 - self.bits[(k + 2) % COLORS]
            self.copy_b(u, k).wait_recv()
            total = self.two(u, k, self.index(k, a, b, away)) + self.ra[slot, k, 2 * b + away].astype(F32)
            self.sc[slot, k, 0] = (total + self.rb[slot, k, away].astype(F32)).astype(BF)
            self.copy_c(u, k).start()

    def phase_d(self, u):
        slot = lax.rem(u, IN)

        @pl.when(u >= IN)
        def _():
            self.write(u - IN).wait()

        for k in range(COLORS):
            b, c = self.bits[(k + 1) % COLORS], self.bits[(k + 2) % COLORS]
            self.copy_c(u, k).wait_recv()
            total = self.two(u, k, self.chip) + self.ra[slot, k, 2 * b + c].astype(F32)
            total = total + self.rb[slot, k, c].astype(F32) + self.rc[slot, k, 0].astype(F32)
            rounded = total.astype(BF)
            self.out[slot, pl.ds(PIECE * k, PIECE), :] = rounded
            wide = rounded.astype(F32)
            square = wide * wide
            self.squares[:] += square[0:8] + square[8:16] + square[16:24] + square[24:PIECE]
        self.write(u).start()
        self.copy_0(u).wait_send()
        for k in range(COLORS):
            self.copy_a(u, k).wait_send()
            self.copy_b(u, k).wait_send()
            self.copy_c(u, k).wait_send()

        @pl.when(u + IN < UNITS)
        def _():
            pl.semaphore_signal(self.free.at[3], inc=1, device_id={"dp": self.partner}, device_id_type=MESH)
            for axis in range(COLORS):
                pl.semaphore_signal(self.free.at[axis], inc=1, device_id={"dp": self.near[axis]}, device_id_type=MESH)

    def tick(self, q, low, high):
        for lag, phase in zip(LAGS, (self.phase_d, self.phase_c, self.phase_b, self.phase_a, self.phase_0)):
            u = q - lag

            @pl.when((u >= low) & (u < high))
            def _(phase=phase, u=u):
                phase(u)


class Gather:
    def __init__(self, wide, down, sems):
        self.wide, self.down, self.sems = wide, down, sems
        self.core, _, self.bits, self.partner, self.near = place()

    def by_kind(self, n, do, kinds=WIDE + DOWN, when=True):
        layer, at = n // 19, lax.rem(n, 19)

        def wide(chips, core, color=None):
            rows = pl.ds(0, FEW) if color is None else pl.ds(PIECE * color, PIECE)
            return self.wide.at[2 * layer + lax.rem(at, 2), *chips, core, rows, span(at // 2, BLOCK)]

        def down(chips, core, color=None):
            rows = pl.ds(0, HALF) if color is None else pl.ds(88 * color, (88, 88, 80)[color])
            return self.down.at[layer, *chips, core, rows, span((at - 16), BLOCK)]

        inside = (n >= 0) & (n < GATHERS) & when
        for kind, piece in (("wide", wide), ("down", down)):
            if kind in kinds:
                mine = True if len(kinds) == 1 else at < 16 if kind == "wide" else at >= 16
                pl.when(inside & mine)(functools.partial(do, piece))

    def copy(self, phase, n, k, at, device):
        send, recv = self.sems[phase]
        slot = lax.rem(n, SLOTS)
        return pltpu.make_async_remote_copy(
            src_ref=at, dst_ref=at, send_sem=send.at[slot, k], recv_sem=recv.at[slot, k], device_id={"dp": device}, device_id_type=MESH
        )

    def copies(self, phase, n, piece, coming=False):
        found = []
        for k in range(COLORS):
            order = (k, (k + 1) % COLORS, (k + 2) % COLORS)
            chips = list(self.bits)
            if coming:
                chips[order[phase]] = 1 - chips[order[phase]]
            for axis in order[:phase]:
                chips[axis] = slice(None)
            found.append(self.copy(phase, n, k, piece(chips, self.core, k), self.near[order[phase]]))
        return found

    def across(self, n, piece, core):
        return self.copy(3, n, 0, piece([slice(None)] * 3, core), self.partner)

    def first(self, n, kinds=WIDE + DOWN, when=True):
        def do(piece):
            for c in self.copies(0, n, piece):
                c.start()

        self.by_kind(n, do, kinds, when)

    def hop(self, phase, n, kinds, when):
        def do(piece):
            for c in self.copies(phase - 1, n, piece, coming=True):
                c.wait_recv()
            for c in self.copies(phase, n, piece):
                c.start()

        self.by_kind(n, do, kinds, when)

    def middle(self, n, kinds=WIDE + DOWN, when=True):
        self.hop(1, n, kinds, when)

    def last(self, n, kinds=WIDE + DOWN, when=True):
        self.hop(2, n, kinds, when)

    def send(self, n, kinds=WIDE + DOWN):
        self.first(n + 4, kinds, n + 4 <= HURRY)
        self.middle(n + 2, kinds, n + 2 <= HURRY)
        self.last(n, kinds, n <= HURRY)

    def share(self, n, kinds=WIDE + DOWN):
        def do(piece):
            for c in self.copies(2, n, piece, coming=True):
                c.wait_recv()
            self.across(n, piece, self.core).start()
            for phase in range(COLORS):
                for c in self.copies(phase, n, piece):
                    c.wait_send()

        self.by_kind(n, do, kinds)

    def arrive(self, n, kinds=WIDE + DOWN):
        def do(piece):
            self.across(n, piece, 1 - self.core).wait_recv()
            self.across(n, piece, self.core).wait_send()

        self.by_kind(n, do, kinds)


class Plan:
    def __init__(self):
        self.first, self.low, self.made, self.log = LAST, 0, 0, []

    def stage(self, at, steps, units_before):
        stage = (self.first, self.low, self.made)
        for j in range(steps):
            if j in at:
                self.log.append((self.first, self.low, self.made + units_before(j)))
                self.first += 1
            for u in range(self.made + units_before(j), self.made + units_before(j + 1)):
                assert u - OWN < self.low or u - OWN <= self.log[-1][0] - LAST, u
        self.made += units_before(steps)
        return stage

    def restart(self, idle):
        assert self.first - LAST >= self.made, (self.first, self.made)
        self.first, self.low = self.made - idle, self.made

    def check(self):
        seen = {}
        for q, low, high in self.log:
            for name, lag in zip("dcba0", LAGS):
                u = q - lag
                if low <= u < high:
                    seen.setdefault(u, []).append(name)
        assert all(seen.get(u) == list("0abcd") for u in range(UNITS)), seen


def step_kernel(
    x, dy, w_gate, w_up, w_down,
    wide, down, g_all, u_all, act_all, a_all, h1, d_all, g_hbm, total_ref,
    x1, own, r0, ra, rb, rc, sa, sb, sc, out, squares, sums, sum_all,
    s0s, s0r, sas, sar, sbs, sbr, scs, scr, out_sem, free, sum_send, sum_recv, load_sem, act_sem, own_sem,
    *gather_sems,
):
    me = lax.axis_index("dp")
    barrier = pltpu.get_barrier_semaphore()
    for other in range(1, DEVICES):
        pl.semaphore_signal(barrier, inc=1, device_id={"dp": (me + other) % DEVICES}, device_id_type=MESH)
    pl.semaphore_wait(barrier, 15)

    gather = Gather(wide, down, tuple(zip(gather_sems[::2], gather_sems[1::2])))
    scatter = Scatter(own, r0, ra, rb, rc, sa, sb, sc, out, squares, ((s0s, s0r), (sas, sar), (sbs, sbr), (scs, scr), out_sem), free, g_hbm)
    squares[:] = jnp.zeros_like(squares)
    load = pltpu.make_async_copy(dy, x1, load_sem.at[0])

    def own_blocks(gate, up, low, then):
        taken = [pltpu.make_async_copy(a, b, own_sem.at[i]) for i, (a, b) in enumerate(((w_gate, gate), (w_up, up), (w_down, low)))]
        for c in taken:
            c.start()
        at, put = (*gather.bits, gather.core), []
        for i, held in enumerate((gate, up, low)):
            taken[i].wait()
            for layer in BOTH:
                to = down.at[layer, *at] if i == 2 else wide.at[2 * layer + i, *at]
                put.append(pltpu.make_async_copy(held.at[layer], to, own_sem.at[3 + 2 * i + layer]))
                put[-1].start()
        for c in put[0::2]:
            c.wait()
        then()
        for c in put[1::2]:
            c.wait()

    def norm(a):
        def some(i):
            at = span(i, ROWS)
            a[at, :] = normed(x1[at, :])

        loop(0, M // ROWS, some)

    def up_and_gate(a, layer, aside):
        unit, second = 19 * layer, layer > 0
        gather.share(unit + 1, WIDE)
        gather.arrive(unit, WIDE)
        gather.arrive(unit + 1, WIDE)

        def step(wg_ref, wu_ref, g_ref, u_ref, act_ref):
            c, m = ids(2)
            following = unit + 2 * c + 2

            @pl.when(((m == 0) | (m == 3)) & (c < 6))
            def _():
                gather.send(following + 3 + m // 3)

            @pl.when((m == 3) & (c > 5) & ~second)
            def _():
                gather.send(11 + c)

            @pl.when(second & (c == 5) & (m == 0))
            def _():
                for late in range(HURRY + 1, GATHERS):
                    gather.first(late, DOWN)

            @pl.when(second & (c == 7) & (m < 3))
            def _():
                gather.middle(HURRY + 1 + m, DOWN)

            @pl.when((m == 1) & (c < 7))
            def _():
                gather.share(following, WIDE)
                gather.share(following + 1, WIDE)

            @pl.when((m == 2) & (c == 7) & ~second)
            def _():
                gather.share(c + 9, DOWN)

            @pl.when((m == 3) & (c == 2))
            def _():
                aside()

            for s in BOTH:
                rows = pl.ds(HALF * s, HALF)
                mine = a[pl.ds(pl.multiple_of(m * BLOCK, BLOCK) + HALF * s, HALF), :]
                gate = jnp.dot(mine, wg_ref[:].reshape(D, BLOCK), preferred_element_type=F32)
                g_ref[rows, :] = gate
                up = jnp.dot(mine, wu_ref[:].reshape(D, BLOCK), preferred_element_type=F32)
                u_ref[rows, :] = up
                act_ref[rows, :] = (gate * lax.logistic(gate) * up).astype(BF)

            @pl.when((m == 2) & (c < 7))
            def _():
                gather.arrive(following, WIDE)
                gather.arrive(following + 1, WIDE)

        weight = pl.BlockSpec((*SPREAD, FEW, BLOCK), lambda c, m: (*ZEROS, c))
        tile = pl.BlockSpec((BLOCK, BLOCK), lambda c, m: (m, c))
        pltpu.emit_pipeline(step, grid=(8, 4), in_specs=[weight, weight], out_specs=[tile] * 3)(
            wide.at[2 * layer], wide.at[2 * layer + 1], g_all.at[layer], u_all.at[layer], act_all.at[layer]
        )

    def lower():
        def step(act_ref, w_ref):
            p, m = ids(2)

            @pl.when(m == 0)
            def _():
                gather.send(19 + p, WIDE)

            @pl.when((p == 2) & (m > 1))
            def _():
                gather.send(20 + m, WIDE)

            @pl.when((m == 1) & (p < 2))
            def _():
                gather.share(17 + p, DOWN)

            columns = span(p, BLOCK)
            for s in BOTH:
                w = w_ref[:].reshape(F, BLOCK)
                by = jnp.dot(act_ref[HALF * s : HALF * s + HALF, :], w, preferred_element_type=F32).astype(BF)
                rows = pl.ds(pl.multiple_of(m * BLOCK, BLOCK) + HALF * s, HALF)
                x1[rows, columns] = (x1[rows, columns].astype(F32) + by.astype(F32)).astype(BF)

            @pl.when((m == 2) & (p < 2))
            def _():
                gather.arrive(17 + p, DOWN)

        gather.arrive(16, DOWN)
        weight = pl.BlockSpec((*SPREAD, TALL, BLOCK), lambda p, m: (*ZEROS, p))
        pltpu.emit_pipeline(step, grid=(3, 4), in_specs=[pl.BlockSpec((BLOCK, F), lambda p, m: (m, 0)), weight], out_specs=[])(
            act_all.at[0], down.at[0]
        )

    def forward(x2):
        take = pltpu.make_async_copy(x, x1, load_sem.at[0])
        take.start()
        keep_h1 = pltpu.make_async_copy(x1, h1, load_sem.at[2])

        def begin(i):
            gather.send(i, WIDE)

        def then():
            gather.first(0, WIDE)
            gather.first(1, WIDE)

        def own(gate, up, low):
            own_blocks(gate, up, low, then)

        with jax.named_scope("begin"):
            pl.run_scoped(own, pltpu.VMEM((2, FEW, F), BF), pltpu.VMEM((2, FEW, F), BF), pltpu.VMEM((2, HALF, D), BF))
            for unit in BOTH:
                gather.first(unit + 2, WIDE)
                gather.middle(unit, WIDE)
            take.wait()
            norm(x2)
            loop(0, 5, begin)
            gather.share(0, WIDE)

        def layer(number):
            keep_a = pltpu.make_async_copy(x2, a_all.at[number], load_sem.at[1])
            keep_a.start()

            def aside():
                keep_a.wait()

                @pl.when(number == 1)
                def _():
                    keep_h1.wait()
                    load.start()

            with jax.named_scope("up_and_gate"):
                up_and_gate(x2, number, aside)

            @pl.when(number == 0)
            def _():
                with jax.named_scope("lower"):
                    lower()
                with jax.named_scope("norm"):
                    gather.share(19, WIDE)
                    norm(x2)
                keep_h1.start()


        loop(0, 2, layer)

    def down_gradient(layer, made, stage):
        def body(held):
            def block(f):
                return pltpu.make_async_copy(
                    act_all.at[layer, :, span(f, BLOCK)], held.at[f], act_sem.at[f]
                )

            for f in range(8):
                block(f).start()
            second = layer > 0
            pl.when(second)(load.wait)

            def step(t):
                third, quarter = t // 4, lax.rem(t, 4)

                @pl.when(second & (t < 3))
                def _():
                    gather.last(HURRY + 1 + t, DOWN)

                @pl.when(second & ((t == 5) | (t == 8) | (t == 11)))
                def _():
                    gather.share(HURRY + t // 3, DOWN)

                @pl.when(t < 4)
                def _():
                    block(2 * quarter).wait()
                    block(2 * quarter + 1).wait()

                @pl.when(lax.rem(t, 2) == 0)
                def _():
                    scatter.tick(stage[0] + t // 2, stage[1], stage[2] + third * 8 // 3)

                for b in BOTH:
                    f = 2 * quarter + b
                    tile = dot(held[f], x1[:, span(third, BLOCK)], TN).astype(BF)
                    for rows in range(8):
                        piece = third * 8 + rows
                        for core in BOTH:
                            row = HALF * core + PIECE * rows
                            own[lax.rem(made + piece // 3, OWN), core, f, lax.rem(piece, 3), :, :] = tile[row : row + PIECE, :]

            loop(0, 12, step)

        pl.run_scoped(body, pltpu.VMEM((8, M, BLOCK), BF))

    def hidden(x2, layer, made, stage):
        def step(w_ref, g_ref, u_ref, dg_ref, du_ref):
            f, phase = ids(2)
            seen = stage[2] + 2 * f

            @pl.when((phase == 0) | (phase == 2) | ((phase == 3) & ((f == 0) | (f == 2))))
            def _():
                at = 5 * (f // 2) + 3 * lax.rem(f, 2) + phase - phase // 2
                at = jnp.where(f < 4, at, 2 + 2 * f + phase // 2)
                scatter.tick(stage[0] + at, stage[1], seen + phase // 3)

            @pl.when(phase < 2)
            def _():
                for s in range(4):
                    rows = pl.ds(HALF * s, HALF)
                    here = span(4 * phase + s, HALF)
                    by = dot(x1[here, :], w_ref[:].reshape(BLOCK, D), NT).astype(BF).astype(F32)
                    gate, up = g_ref[rows, :], u_ref[rows, :]
                    sigmoid = lax.logistic(gate)
                    silu = gate * sigmoid
                    du_ref[here, :] = (by * silu).astype(BF)
                    dg_ref[here, :] = (by * up * (sigmoid + silu * (1.0 - sigmoid))).astype(BF)

            def unit(by_ref, which):
                slot = lax.rem(made + 2 * f + which, OWN)
                for b in range(4):
                    tile = dot(x2[:, FOURTH * b : FOURTH * b + FOURTH], by_ref[:], TN).astype(BF)
                    for s in range(4):
                        for k in range(COLORS):
                            row = FEW * s + PIECE * k
                            own[slot, s % 2, 2 * b + s // 2, k, :, :] = tile[row : row + PIECE, :]

            pl.when(phase == 2)(lambda: unit(dg_ref, 0))
            pl.when(phase == 3)(lambda: unit(du_ref, 1))

        tile = pl.BlockSpec((WIDTH, BLOCK), lambda f, phase: (jnp.minimum(phase, 1), f), pipeline_mode=pl.Buffered(3))
        all_rows = pl.BlockSpec((M, BLOCK), lambda f, phase: (0, f))
        weight = pl.BlockSpec((1, 1, 1, 2, HALF, D), lambda f, phase: (*bits_of(f), *ZEROS[:3]))
        pltpu.emit_pipeline(step, grid=(8, 4), in_specs=[weight, tile, tile], out_specs=[all_rows, all_rows])(
            down.at[layer], g_all.at[layer], u_all.at[layer], d_all.at[0, layer], d_all.at[1, layer]
        )

    def states(stage):
        def body(da, held):
            def step(d_ref, w_ref):
                m, which, n = ids(3)
                first, end = (which == 0) & (n == 0), (which == 1) & (n == 1)
                take = pltpu.make_async_copy(h1.at[span(m, BLOCK)], held, load_sem.at[2])

                @pl.when(first)
                def _():
                    take.start()

                scatter.tick(stage[0] + 4 * m + 2 * which + n, stage[1], stage[2])
                by = dot(d_ref[:].reshape(BLOCK, F), w_ref[:].reshape(768, F), NT).astype(BF)

                @pl.when(which == 0)
                def _():
                    da[n] = by

                @pl.when(which > 0)
                def _():
                    da[n] = (da[n].astype(F32) + by.astype(F32)).astype(BF)

                @pl.when(end)
                def _():
                    take.wait()

                    def some(i):
                        at = span(i, ROWS)
                        wide = held[at, :].astype(F32)
                        scale = lax.rsqrt(along(jnp.mean, wide * wide) + 1e-6)
                        by = jnp.concatenate([da[n, at, :] for n in BOTH], axis=-1).astype(F32)
                        inner = along(jnp.sum, by * wide)
                        back = (by * scale - wide * (inner * scale * scale * scale * (1.0 / D))).astype(BF)
                        at_all = span(8 * m + i, ROWS)
                        x1[at_all, :] = (x1[at_all, :].astype(F32) + back.astype(F32)).astype(BF)

                    loop(0, 8, some)

            tile = pl.BlockSpec((1, BLOCK, F), lambda m, which, n: (which, m, 0))
            rows = pl.BlockSpec((1, 1, *SPREAD[:3], FEW, F), lambda m, which, n: (2 + which, n, *ZEROS))
            pltpu.emit_pipeline(step, grid=(4, 2, 2), in_specs=[tile, rows], out_specs=[])(d_all.at[:, 1], wide)

        pl.run_scoped(body, pltpu.VMEM((2, BLOCK, 768), BF), pltpu.VMEM((BLOCK, D), BF))

    plan, stages = Plan(), {}
    for layer in (1, 0):
        plan.restart(2)
        stages["down", layer] = plan.stage(range(0, 12, 2), 12, lambda t: t // 4 * 8 // 3)
        at = [4 * f + phase for f in range(8) for phase in ((0, 2, 3) if f in (0, 2) else (0, 2))]
        stages["hidden", layer] = plan.stage(at, PIECE, lambda j: j // 4 * 2 + j % 4 // 3)
        if layer:
            stages["states"] = plan.stage(range(16), 16, lambda j: 0)
    left = UNITS + LAST - plan.first
    first_left, low_left, _ = plan.stage(range(left), left, lambda j: 0)
    plan.check()

    def backward(i):
        layer, made = 1 - i, 24 * i

        def chosen(name):
            return tuple(jnp.where(i == 0, a, b) for a, b in zip(stages[name, 1], stages[name, 0]))

        def gradients(x2):
            take = pltpu.make_async_copy(a_all.at[layer], x2, load_sem.at[1])
            take.start()
            with jax.named_scope("down_gradient"):
                down_gradient(layer, made, chosen("down"))

            @pl.when(layer == 1)
            def _():
                def one(n):
                    gather.arrive(n, DOWN)

                loop(35, 38, one)

            take.wait()
            with jax.named_scope("hidden"):
                hidden(x2, layer, made + 8, chosen("hidden"))

        pl.run_scoped(gradients, pltpu.VMEM((M, D), BF))
        @pl.when(layer == 1)
        def _():
            with jax.named_scope("states"):
                states(stages["states"])


    pl.run_scoped(forward, pltpu.VMEM((M, D), BF))
    loop(0, 2, backward)

    def rest(t):
        scatter.tick(first_left + t, low_left, UNITS)

    with jax.named_scope("rest"):
        loop(0, left, rest)

    def last(u):
        scatter.write(u).wait()

    loop(UNITS - IN, UNITS, last)

    mine = jnp.sum(squares[:], axis=(0, 1), keepdims=True)
    sums[:] = jnp.broadcast_to(mine, sums.shape)

    def tell(to, of):
        return pltpu.make_async_remote_copy(
            src_ref=sums, dst_ref=sum_all.at[of], send_sem=sum_send.at[to], recv_sem=sum_recv.at[of], device_id={"dp": to}, device_id_type=MESH
        )

    for other in range(1, DEVICES):
        tell((me + other) % DEVICES, me).start()
    for other in range(1, DEVICES):
        tell((me + other) % DEVICES, (me + other) % DEVICES).wait_recv()
    for other in range(1, DEVICES):
        tell((me + other) % DEVICES, me).wait_send()
    sum_all[me] = sums[:]
    total = sum_all[0]
    for i in range(1, DEVICES):
        total = total + sum_all[i]
    total_ref[:] = total


def one_step(*args):
    any_spec = pl.BlockSpec(memory_space=pl.ANY)
    shape = jax.ShapeDtypeStruct
    piece = (COLORS, PIECE, BLOCK)
    dma = pltpu.SemaphoreType.DMA
    sums = [pltpu.VMEM((IN, COLORS, n, PIECE, BLOCK), BF) for n in (4, 2, 1)]
    outs = [
        shape((4, *SPREAD, FEW, F), BF), shape((LAYERS, *SPREAD, TALL, D), BF), shape((LAYERS, M, F), F32), shape((LAYERS, M, F), F32),
        shape((LAYERS, M, F), BF), shape((LAYERS, M, D), BF), shape((M, D), BF), shape((CORES, LAYERS, M, F), BF),
    ]
    outs = pl.pallas_call(
        step_kernel,
        out_shape=[*outs, shape((UNITS, FEW, BLOCK), BF), shape(TILE, F32)],
        in_specs=[any_spec] * 5,
        out_specs=[any_spec] * (len(outs) + 1) + [pl.BlockSpec(memory_space=pltpu.VMEM)],
        scratch_shapes=[
            pltpu.VMEM((M, D), BF),
            pltpu.VMEM((OWN, CORES, 8, *piece), BF),
            pltpu.VMEM((IN, 8, *piece), BF), *sums, *sums,
            pltpu.VMEM((IN, FEW, BLOCK), BF), pltpu.VMEM((8, BLOCK), F32), pltpu.VMEM(TILE, F32), pltpu.VMEM((DEVICES, *TILE), F32),
            dma((IN,)), dma((IN,)), *[dma((IN, COLORS))] * 6, dma((IN,)), pltpu.SemaphoreType.REGULAR((4,)),
            dma((DEVICES,)), dma((DEVICES,)), *[dma((9,))] * 3, *[dma((SLOTS, COLORS))] * 8,
        ],
        compiler_params=pltpu.CompilerParams(collective_id=0, has_side_effects=True, vmem_limit_bytes=VMEM),
        cost_estimate=pl.CostEstimate(flops=15 * 2 * M * D * F, bytes_accessed=900_000_000, transcendentals=0),
        name="training_step",
    )(*args)
    return outs[-2], outs[-1]


def adamw_kernel(total, *refs):
    count = LAYERS * COLORS * D * F
    factor = jnp.minimum(1.0, 0.5 * lax.rsqrt(total[:1, :1] / count + 1e-30))
    for i in range(COLORS):
        w, m, v, g, new_w, new_m, new_v = refs[i::COLORS]
        blocks = [(b, pl.ds(0, FEW), pl.ds(BLOCK * b, BLOCK)) for b in BOTH]
        if i == 2:
            blocks = [((c, r), pl.ds(PIECE * r, PIECE), pl.ds(BLOCK * c, BLOCK)) for c in range(COLORS) for r in BOTH]
        for at, rows, columns in blocks:
            by = (g[0, at, 0] if i < 2 else g[0, at[0], at[1]]).astype(F32) * factor
            new_w[0, rows, columns], new_m[0, rows, columns], new_v[0, rows, columns] = adamw(
                w[0, rows, columns].astype(F32), m[0, rows, columns], v[0, rows, columns], by
            )


def optimizer(total, weights, m, v, units):
    wide = pl.BlockSpec((1, FEW, WIDTH), lambda layer, i: (layer, 0, i))
    down = pl.BlockSpec((1, ROWS, D), lambda layer, i: (layer, i, 0))
    blocks = [wide, wide, down]

    def order(which):
        return lambda layer, i: (1 - layer, 2 + i, which, 0, 0)

    gradients = [pl.BlockSpec((1, 2, 1, FEW, BLOCK), order(0)), pl.BlockSpec((1, 2, 1, FEW, BLOCK), order(1))]
    gradients.append(pl.BlockSpec((1, 3, 2, PIECE, BLOCK), lambda layer, i: (1 - layer, 0, i, 0, 0)))
    by_columns, by_rows = units.reshape(2, 12, 2, FEW, BLOCK), units.reshape(2, 9, 8, PIECE, BLOCK)
    return pl.pallas_call(
        adamw_kernel,
        grid=(2, 4),
        out_shape=[jax.ShapeDtypeStruct(w.shape, BF) for w in weights] + [jax.ShapeDtypeStruct(a.shape, F32) for a in (*m, *v)],
        in_specs=[pl.BlockSpec(TILE, lambda layer, i: (0, 0)), *blocks * 3, *gradients],
        out_specs=blocks * 3,
        compiler_params=pltpu.CompilerParams(vmem_limit_bytes=VMEM),
        name="optimizer",
    )(total, *weights, *m, *v, by_columns, by_columns, by_rows)


def solution(mesh):
    def step(x, dy, *arrays):
        weights, m, v = (arrays[i : i + 3] for i in (0, 3, 6))
        units, total = one_step(x[0], dy[0], *weights)
        return tuple(optimizer(total, weights, m, v, units))

    states, cut = P(("rep", "dp"), None, None), P(None, "dp", None)
    return jax.shard_map(
        step,
        mesh=mesh,
        in_specs=(states, states) + (cut,) * 9,
        out_specs=(P("rep", "dp", None),) * 9,
        check_vma=False,
    )
```

```python
import functools

import jax
import jax.numpy as jnp
from jax import lax
from jax.experimental import pallas as pl
from jax.experimental.pallas import tpu as pltpu
from jax.sharding import PartitionSpec as P

NAMES = ("w_gate", "w_up", "w_down")
BF, F32 = jnp.bfloat16, jnp.float32
MESH = pl.DeviceIdType.MESH
TN = (((0,), (0,)), ((), ()))
NT = (((1,), (1,)), ((), ()))
M, D, F = 2048, 1536, 4096
BLOCK, HALF, QUARTER = 512, 256, 128
PIECE, FEW, TALL = 32, 96, 256
COLORS, CORES, LAYERS, ROWS, DEVICES = 3, 2, 2, 64, 16
WIDTH, FOURTH, TILE = 2 * BLOCK, D // 4, (8, 128)
VMEM = 67_000_000
WEIGHTS = (4, 2, 1)
BOTH = range(CORES)
SPREAD, ZEROS = (CORES,) * 4, (0,) * 5
UNITS = 48
OWN, IN = 8, 6
GATHERS, SLOTS = 38, 10
WIDE, DOWN = ("wide",), ("down",)
HURRY = 34
LAST = 5
LAGS = (LAST, 4, 3, 1, 0)


def span(i, size):
    return pl.ds(pl.multiple_of(i * size, size), size)


def loop(first, last, do):
    def step(i, carry):
        do(i)
        return carry

    lax.fori_loop(first, last, step, 0)


def ids(n):
    return tuple(pl.program_id(i) for i in range(n))


def along(reduce, a):
    return reduce(a, -1, keepdims=True)


def bits_of(chip):
    return tuple(chip // w % 2 for w in WEIGHTS)


def place():
    me = lax.axis_index("dp")
    chip = me // CORES
    bits = bits_of(chip)
    near = tuple(me + CORES * w * (1 - 2 * b) for b, w in zip(bits, WEIGHTS))
    return me % CORES, chip, bits, me + 1 - 2 * (me % CORES), near


def dot(a, b, dims):
    return lax.dot_general(a, b, dims, preferred_element_type=F32)


def normed(h):
    wide = h.astype(F32)
    scale = lax.rsqrt(along(jnp.mean, wide * wide) + 1e-6)
    return (wide * scale).astype(BF)


def adamw(w, m, v, g):
    m = 0.9 * m + 0.1 * g
    v = 0.95 * v + 0.05 * g * g
    step = m * lax.rsqrt(v + 1e-8) + 0.1 * w
    return (w - 0.02 * step).astype(BF), m, v


class Scatter:
    def __init__(self, own, r0, ra, rb, rc, sa, sb, sc, out, squares, sems, free, g_hbm):
        self.own, self.r0, self.ra, self.rb, self.rc = own, r0, ra, rb, rc
        self.sa, self.sb, self.sc, self.out, self.squares = sa, sb, sc, out, squares
        self.sems, self.free, self.g_hbm = sems, free, g_hbm
        self.core, self.chip, self.bits, self.partner, self.near = place()

    def copy(self, phase, src, dst, slot, color, device):
        send, recv = self.sems[phase]
        at = (slot,) if color is None else (slot, color)
        return pltpu.make_async_remote_copy(
            src_ref=src, dst_ref=dst, send_sem=send.at[at], recv_sem=recv.at[at], device_id={"dp": device}, device_id_type=MESH
        )

    def copy_0(self, u):
        slot = lax.rem(u, IN)
        return self.copy(0, self.own.at[lax.rem(u, OWN), 1 - self.core], self.r0.at[slot], slot, None, self.partner)

    def copy_a(self, u, k):
        slot = lax.rem(u, IN)
        return self.copy(1, self.sa.at[slot, k], self.ra.at[slot, k], slot, k, self.near[k])

    def copy_b(self, u, k):
        slot = lax.rem(u, IN)
        return self.copy(2, self.sb.at[slot, k], self.rb.at[slot, k], slot, k, self.near[(k + 1) % COLORS])

    def copy_c(self, u, k):
        slot = lax.rem(u, IN)
        return self.copy(3, self.sc.at[slot, k], self.rc.at[slot, k], slot, k, self.near[(k + 2) % COLORS])

    def write(self, u):
        slot = lax.rem(u, IN)
        return pltpu.make_async_copy(self.out.at[slot], self.g_hbm.at[u], self.sems[4].at[slot])

    def index(self, k, a, b, c):
        return a * WEIGHTS[k] + b * WEIGHTS[(k + 1) % COLORS] + c * WEIGHTS[(k + 2) % COLORS]

    def two(self, u, k, index):
        own = self.own[lax.rem(u, OWN), self.core, index, k].astype(F32)
        return own + self.r0[lax.rem(u, IN), index, k].astype(F32)

    def phase_0(self, u):
        @pl.when(u >= IN)
        def _():
            pl.semaphore_wait(self.free.at[3], 1)

        self.copy_0(u).start()

    def phase_a(self, u):
        @pl.when(u >= IN)
        def _():
            for axis in range(COLORS):
                pl.semaphore_wait(self.free.at[axis], 1)

        self.copy_0(u).wait_recv()
        slot = lax.rem(u, IN)
        for k in range(COLORS):
            away = 1 - self.bits[k]
            for b in BOTH:
                for c in BOTH:
                    self.sa[slot, k, 2 * b + c] = self.two(u, k, self.index(k, away, b, c)).astype(BF)
            self.copy_a(u, k).start()

    def phase_b(self, u):
        slot = lax.rem(u, IN)
        for k in range(COLORS):
            here, away = self.bits[k], 1 - self.bits[(k + 1) % COLORS]
            self.copy_a(u, k).wait_recv()
            for c in BOTH:
                total = self.two(u, k, self.index(k, here, away, c)) + self.ra[slot, k, 2 * away + c].astype(F32)
                self.sb[slot, k, c] = total.astype(BF)
            self.copy_b(u, k).start()

    def phase_c(self, u):
        slot = lax.rem(u, IN)
        for k in range(COLORS):
            a, b, away = self.bits[k], self.bits[(k + 1) % COLORS], 1 - self.bits[(k + 2) % COLORS]
            self.copy_b(u, k).wait_recv()
            total = self.two(u, k, self.index(k, a, b, away)) + self.ra[slot, k, 2 * b + away].astype(F32)
            self.sc[slot, k, 0] = (total + self.rb[slot, k, away].astype(F32)).astype(BF)
            self.copy_c(u, k).start()

    def phase_d(self, u):
        slot = lax.rem(u, IN)

        @pl.when(u >= IN)
        def _():
            self.write(u - IN).wait()

        for k in range(COLORS):
            b, c = self.bits[(k + 1) % COLORS], self.bits[(k + 2) % COLORS]
            self.copy_c(u, k).wait_recv()
            total = self.two(u, k, self.chip) + self.ra[slot, k, 2 * b + c].astype(F32)
            total = total + self.rb[slot, k, c].astype(F32) + self.rc[slot, k, 0].astype(F32)
            rounded = total.astype(BF)
            self.out[slot, pl.ds(PIECE * k, PIECE), :] = rounded
            wide = rounded.astype(F32)
            square = wide * wide
            self.squares[:] += square[0:8] + square[8:16] + square[16:24] + square[24:PIECE]
        self.write(u).start()
        self.copy_0(u).wait_send()
        for k in range(COLORS):
            self.copy_a(u, k).wait_send()
            self.copy_b(u, k).wait_send()
            self.copy_c(u, k).wait_send()

        @pl.when(u + IN < UNITS)
        def _():
            pl.semaphore_signal(self.free.at[3], inc=1, device_id={"dp": self.partner}, device_id_type=MESH)
            for axis in range(COLORS):
                pl.semaphore_signal(self.free.at[axis], inc=1, device_id={"dp": self.near[axis]}, device_id_type=MESH)

    def tick(self, q, low, high):
        for lag, phase in zip(LAGS, (self.phase_d, self.phase_c, self.phase_b, self.phase_a, self.phase_0)):
            u = q - lag

            @pl.when((u >= low) & (u < high))
            def _(phase=phase, u=u):
                phase(u)


class Gather:
    def __init__(self, wide, down, sems):
        self.wide, self.down, self.sems = wide, down, sems
        self.core, _, self.bits, self.partner, self.near = place()

    def by_kind(self, n, do, kinds=WIDE + DOWN, when=True):
        layer, at = n // 19, lax.rem(n, 19)

        def wide(chips, core, color=None):
            rows = pl.ds(0, FEW) if color is None else pl.ds(PIECE * color, PIECE)
            return self.wide.at[2 * layer + lax.rem(at, 2), *chips, core, rows, span(at // 2, BLOCK)]

        def down(chips, core, color=None):
            rows = pl.ds(0, HALF) if color is None else pl.ds(88 * color, (88, 88, 80)[color])
            return self.down.at[layer, *chips, core, rows, span((at - 16), BLOCK)]

        inside = (n >= 0) & (n < GATHERS) & when
        for kind, piece in (("wide", wide), ("down", down)):
            if kind in kinds:
                mine = True if len(kinds) == 1 else at < 16 if kind == "wide" else at >= 16
                pl.when(inside & mine)(functools.partial(do, piece))

    def copy(self, phase, n, k, at, device, source=None):
        send, recv = self.sems[phase]
        slot = lax.rem(n, SLOTS)
        return pltpu.make_async_remote_copy(
            src_ref=at if source is None else source, dst_ref=at, send_sem=send.at[slot, k], recv_sem=recv.at[slot, k], device_id={"dp": device}, device_id_type=MESH
        )

    def copies(self, phase, n, piece, coming=False):
        found = []
        for k in range(COLORS):
            order = (k, (k + 1) % COLORS, (k + 2) % COLORS)
            chips = list(self.bits)
            if coming:
                chips[order[phase]] = 1 - chips[order[phase]]
            for axis in order[:phase]:
                chips[axis] = slice(None)
            found.append(self.copy(phase, n, k, piece(chips, self.core, k), self.near[order[phase]]))
        return found

    def across(self, n, piece, core):
        return self.copy(3, n, 0, piece([slice(None)] * 3, core), self.partner)

    def first(self, n, kinds=WIDE + DOWN, when=True):
        def do(piece):
            for c in self.copies(0, n, piece):
                c.start()

        self.by_kind(n, do, kinds, when)

    def begin(self, n, source):
        for k in range(COLORS):
            at = self.wide.at[n, *self.bits, self.core, pl.ds(PIECE * k, PIECE), pl.ds(0, BLOCK)]
            self.copy(0, n, k, at, self.near[k], source.at[0, pl.ds(PIECE * k, PIECE), pl.ds(0, BLOCK)]).start()

    def hop(self, phase, n, kinds, when):
        def do(piece):
            for c in self.copies(phase - 1, n, piece, coming=True):
                c.wait_recv()
            for c in self.copies(phase, n, piece):
                c.start()

        self.by_kind(n, do, kinds, when)

    def middle(self, n, kinds=WIDE + DOWN, when=True):
        self.hop(1, n, kinds, when)

    def last(self, n, kinds=WIDE + DOWN, when=True):
        self.hop(2, n, kinds, when)

    def send(self, n, kinds=WIDE + DOWN):
        self.first(n + 4, kinds, n + 4 <= HURRY)
        self.middle(n + 2, kinds, n + 2 <= HURRY)
        self.last(n, kinds, n <= HURRY)

    def share(self, n, kinds=WIDE + DOWN):
        def do(piece):
            for c in self.copies(2, n, piece, coming=True):
                c.wait_recv()
            self.across(n, piece, self.core).start()
            for phase in range(COLORS):
                for c in self.copies(phase, n, piece):
                    c.wait_send()

        self.by_kind(n, do, kinds)

    def arrive(self, n, kinds=WIDE + DOWN):
        def do(piece):
            self.across(n, piece, 1 - self.core).wait_recv()
            self.across(n, piece, self.core).wait_send()

        self.by_kind(n, do, kinds)


class Plan:
    def __init__(self):
        self.first, self.low, self.made, self.log = LAST, 0, 0, []

    def stage(self, at, steps, units_before):
        stage = (self.first, self.low, self.made)
        for j in range(steps):
            if j in at:
                self.log.append((self.first, self.low, self.made + units_before(j)))
                self.first += 1
            for u in range(self.made + units_before(j), self.made + units_before(j + 1)):
                assert u - OWN < self.low or u - OWN <= self.log[-1][0] - LAST, u
        self.made += units_before(steps)
        return stage

    def restart(self, idle):
        assert self.first - LAST >= self.made, (self.first, self.made)
        self.first, self.low = self.made - idle, self.made

    def check(self):
        seen = {}
        for q, low, high in self.log:
            for name, lag in zip("dcba0", LAGS):
                u = q - lag
                if low <= u < high:
                    seen.setdefault(u, []).append(name)
        assert all(seen.get(u) == list("0abcd") for u in range(UNITS)), seen


def step_kernel(
    x, dy, w_gate, w_up, w_down,
    wide, down, g_all, u_all, act_all, a_all, h1, d_all, g_hbm, total_ref,
    x1, own, r0, ra, rb, rc, sa, sb, sc, out, squares, sums, sum_all,
    s0s, s0r, sas, sar, sbs, sbr, scs, scr, out_sem, free, sum_send, sum_recv, load_sem, act_sem, own_sem,
    *gather_sems,
):
    me = lax.axis_index("dp")
    barrier = pltpu.get_barrier_semaphore()
    for other in range(1, DEVICES):
        pl.semaphore_signal(barrier, inc=1, device_id={"dp": (me + other) % DEVICES}, device_id_type=MESH)
    pl.semaphore_wait(barrier, 15)

    gather = Gather(wide, down, tuple(zip(gather_sems[::2], gather_sems[1::2])))
    scatter = Scatter(own, r0, ra, rb, rc, sa, sb, sc, out, squares, ((s0s, s0r), (sas, sar), (sbs, sbr), (scs, scr), out_sem), free, g_hbm)
    squares[:] = jnp.zeros_like(squares)
    load = pltpu.make_async_copy(dy, x1, load_sem.at[0])

    def own_blocks(gate, up, low):
        taken = [pltpu.make_async_copy(a, b, own_sem.at[i]) for i, (a, b) in enumerate(((w_gate, gate), (w_up, up), (w_down, low)))]
        for c in taken:
            c.start()
        at, put = (*gather.bits, gather.core), []
        for i, held in enumerate((gate, up, low)):
            taken[i].wait()
            for layer in BOTH:
                to = down.at[layer, *at] if i == 2 else wide.at[2 * layer + i, *at]
                put.append(pltpu.make_async_copy(held.at[layer], to, own_sem.at[3 + 2 * i + layer]))
                put[-1].start()
        for c in put:
            c.wait()

    def norm(a):
        def some(i):
            at = span(i, ROWS)
            a[at, :] = normed(x1[at, :])

        loop(0, M // ROWS, some)

    def up_and_gate(a, layer, aside):
        unit, second = 19 * layer, layer > 0
        gather.share(unit + 1, WIDE)
        gather.arrive(unit, WIDE)
        gather.arrive(unit + 1, WIDE)

        def step(wg_ref, wu_ref, g_ref, u_ref, act_ref):
            c, m = ids(2)
            following = unit + 2 * c + 2

            @pl.when(((m == 0) | (m == 3)) & (c < 6))
            def _():
                gather.send(following + 3 + m // 3)

            @pl.when((m == 3) & (c > 5) & ~second)
            def _():
                gather.send(11 + c)

            @pl.when(second & (c == 5) & (m == 0))
            def _():
                for late in range(HURRY + 1, GATHERS):
                    gather.first(late, DOWN)

            @pl.when(second & (c == 7) & (m < 3))
            def _():
                gather.middle(HURRY + 1 + m, DOWN)

            @pl.when((m == 1) & (c < 7))
            def _():
                gather.share(following, WIDE)
                gather.share(following + 1, WIDE)

            @pl.when((m == 2) & (c == 7) & ~second)
            def _():
                gather.share(c + 9, DOWN)

            @pl.when((m == 3) & (c == 2))
            def _():
                aside()

            for s in BOTH:
                rows = pl.ds(HALF * s, HALF)
                mine = a[pl.ds(pl.multiple_of(m * BLOCK, BLOCK) + HALF * s, HALF), :]
                gate = jnp.dot(mine, wg_ref[:].reshape(D, BLOCK), preferred_element_type=F32)
                sigmoid = lax.logistic(gate)
                silu = gate * sigmoid
                u_ref[rows, :] = silu
                up = jnp.dot(mine, wu_ref[:].reshape(D, BLOCK), preferred_element_type=F32)
                g_ref[rows, :] = up * (sigmoid + silu * (1.0 - sigmoid))
                act_ref[rows, :] = (silu * up).astype(BF)

            @pl.when((m == 2) & (c < 7))
            def _():
                gather.arrive(following, WIDE)
                gather.arrive(following + 1, WIDE)

        weight = pl.BlockSpec((*SPREAD, FEW, BLOCK), lambda c, m: (*ZEROS, c))
        tile = pl.BlockSpec((BLOCK, BLOCK), lambda c, m: (m, c))
        pltpu.emit_pipeline(step, grid=(8, 4), in_specs=[weight, weight], out_specs=[tile] * 3)(
            wide.at[2 * layer], wide.at[2 * layer + 1], g_all.at[layer], u_all.at[layer], act_all.at[layer]
        )

    def lower():
        def step(act_ref, w_ref):
            p, m = ids(2)

            @pl.when(m == 0)
            def _():
                gather.send(19 + p, WIDE)

            @pl.when((p == 2) & (m > 1))
            def _():
                gather.send(20 + m, WIDE)

            @pl.when((m == 1) & (p < 2))
            def _():
                gather.share(17 + p, DOWN)

            columns = span(p, BLOCK)
            for s in BOTH:
                w = w_ref[:].reshape(F, BLOCK)
                by = jnp.dot(act_ref[HALF * s : HALF * s + HALF, :], w, preferred_element_type=F32).astype(BF)
                rows = pl.ds(pl.multiple_of(m * BLOCK, BLOCK) + HALF * s, HALF)
                x1[rows, columns] = (x1[rows, columns].astype(F32) + by.astype(F32)).astype(BF)

            @pl.when((m == 2) & (p < 2))
            def _():
                gather.arrive(17 + p, DOWN)

        gather.arrive(16, DOWN)
        weight = pl.BlockSpec((*SPREAD, TALL, BLOCK), lambda p, m: (*ZEROS, p))
        pltpu.emit_pipeline(step, grid=(3, 4), in_specs=[pl.BlockSpec((BLOCK, F), lambda p, m: (m, 0)), weight], out_specs=[])(
            act_all.at[0], down.at[0]
        )

    def forward(x2):
        take = pltpu.make_async_copy(x, x1, load_sem.at[0])
        take.start()
        keep_h1 = pltpu.make_async_copy(x1, h1, load_sem.at[2])

        def begin(i):
            gather.send(i, WIDE)

        with jax.named_scope("begin"):
            gather.begin(0, w_gate)
            gather.begin(1, w_up)
            pl.run_scoped(own_blocks, pltpu.VMEM((2, FEW, F), BF), pltpu.VMEM((2, FEW, F), BF), pltpu.VMEM((2, HALF, D), BF))
            for unit in BOTH:
                gather.first(unit + 2, WIDE)
                gather.middle(unit, WIDE)
            take.wait()
            norm(x2)
            loop(0, 5, begin)
            gather.share(0, WIDE)

        def layer(number):
            keep_a = pltpu.make_async_copy(x2, a_all.at[number], load_sem.at[1])
            keep_a.start()

            def aside():
                keep_a.wait()

                @pl.when(number == 1)
                def _():
                    keep_h1.wait()
                    load.start()

            with jax.named_scope("up_and_gate"):
                up_and_gate(x2, number, aside)

            @pl.when(number == 0)
            def _():
                with jax.named_scope("lower"):
                    lower()
                with jax.named_scope("norm"):
                    gather.share(19, WIDE)
                    norm(x2)
                keep_h1.start()


        loop(0, 2, layer)

    def down_gradient(layer, made, stage):
        def body(held):
            def block(f):
                return pltpu.make_async_copy(
                    act_all.at[layer, :, span(f, BLOCK)], held.at[f], act_sem.at[f]
                )

            for f in range(8):
                block(f).start()
            second = layer > 0
            pl.when(second)(load.wait)

            def step(t):
                third, quarter = t // 4, lax.rem(t, 4)

                @pl.when(second & (t < 3))
                def _():
                    gather.last(HURRY + 1 + t, DOWN)

                @pl.when(second & ((t == 5) | (t == 8) | (t == 11)))
                def _():
                    gather.share(HURRY + t // 3, DOWN)

                @pl.when(t < 4)
                def _():
                    block(2 * quarter).wait()
                    block(2 * quarter + 1).wait()

                @pl.when(lax.rem(t, 2) == 0)
                def _():
                    scatter.tick(stage[0] + t // 2, stage[1], stage[2] + third * 8 // 3)

                for b in BOTH:
                    f = 2 * quarter + b
                    tile = dot(held[f], x1[:, span(third, BLOCK)], TN).astype(BF)
                    for rows in range(8):
                        piece = third * 8 + rows
                        for core in BOTH:
                            row = HALF * core + PIECE * rows
                            own[lax.rem(made + piece // 3, OWN), core, f, lax.rem(piece, 3), :, :] = tile[row : row + PIECE, :]

            loop(0, 12, step)

        pl.run_scoped(body, pltpu.VMEM((8, M, BLOCK), BF))

    def hidden(x2, layer, made, stage):
        def step(w_ref, g_ref, u_ref, dg_ref, du_ref):
            f, phase = ids(2)
            seen = stage[2] + 2 * f

            @pl.when((phase == 0) | (phase == 2) | ((phase == 3) & ((f == 0) | (f == 2))))
            def _():
                at = 5 * (f // 2) + 3 * lax.rem(f, 2) + phase - phase // 2
                at = jnp.where(f < 4, at, 2 + 2 * f + phase // 2)
                scatter.tick(stage[0] + at, stage[1], seen + phase // 3)

            @pl.when(phase < 2)
            def _():
                for s in BOTH:
                    rows = pl.ds(BLOCK * s, BLOCK)
                    here = span(CORES * phase + s, BLOCK)
                    by = dot(x1[here, :], w_ref[:].reshape(BLOCK, D), NT).astype(BF).astype(F32)
                    du_ref[here, :] = (by * u_ref[rows, :]).astype(BF)
                    dg_ref[here, :] = (by * g_ref[rows, :]).astype(BF)

            def unit(by_ref, which):
                slot = lax.rem(made + 2 * f + which, OWN)
                for b in range(4):
                    tile = dot(x2[:, FOURTH * b : FOURTH * b + FOURTH], by_ref[:], TN).astype(BF)
                    for s in range(4):
                        for k in range(COLORS):
                            row = FEW * s + PIECE * k
                            own[slot, s % 2, 2 * b + s // 2, k, :, :] = tile[row : row + PIECE, :]

            pl.when(phase == 2)(lambda: unit(dg_ref, 0))
            pl.when(phase == 3)(lambda: unit(du_ref, 1))

        tile = pl.BlockSpec((WIDTH, BLOCK), lambda f, phase: (jnp.minimum(phase, 1), f), pipeline_mode=pl.Buffered(3))
        all_rows = pl.BlockSpec((M, BLOCK), lambda f, phase: (0, f))
        weight = pl.BlockSpec((1, 1, 1, 2, HALF, D), lambda f, phase: (*bits_of(f), *ZEROS[:3]))
        pltpu.emit_pipeline(step, grid=(8, 4), in_specs=[weight, tile, tile], out_specs=[all_rows, all_rows])(
            down.at[layer], g_all.at[layer], u_all.at[layer], d_all.at[0, layer], d_all.at[1, layer]
        )

    def states(stage):
        def body(da, held):
            def step(d_ref, w_ref):
                m, which, n = ids(3)
                first, end = (which == 0) & (n == 0), (which == 1) & (n == 1)
                take = pltpu.make_async_copy(h1.at[span(m, BLOCK)], held, load_sem.at[2])

                @pl.when(first)
                def _():
                    take.start()

                scatter.tick(stage[0] + 4 * m + 2 * which + n, stage[1], stage[2])
                by = dot(d_ref[:].reshape(BLOCK, F), w_ref[:].reshape(768, F), NT).astype(BF)

                @pl.when(which == 0)
                def _():
                    da[n] = by

                @pl.when(which > 0)
                def _():
                    da[n] = (da[n].astype(F32) + by.astype(F32)).astype(BF)

                @pl.when(end)
                def _():
                    take.wait()

                    def some(i):
                        at = span(i, ROWS)
                        wide = held[at, :].astype(F32)
                        scale = lax.rsqrt(along(jnp.mean, wide * wide) + 1e-6)
                        by = jnp.concatenate([da[n, at, :] for n in BOTH], axis=-1).astype(F32)
                        inner = along(jnp.sum, by * wide)
                        back = (by * scale - wide * (inner * scale * scale * scale * (1.0 / D))).astype(BF)
                        at_all = span(8 * m + i, ROWS)
                        x1[at_all, :] = (x1[at_all, :].astype(F32) + back.astype(F32)).astype(BF)

                    loop(0, 8, some)

            tile = pl.BlockSpec((1, BLOCK, F), lambda m, which, n: (which, m, 0))
            rows = pl.BlockSpec((1, 1, *SPREAD[:3], FEW, F), lambda m, which, n: (2 + which, n, *ZEROS))
            pltpu.emit_pipeline(step, grid=(4, 2, 2), in_specs=[tile, rows], out_specs=[])(d_all.at[:, 1], wide)

        pl.run_scoped(body, pltpu.VMEM((2, BLOCK, 768), BF), pltpu.VMEM((BLOCK, D), BF))

    plan, stages = Plan(), {}
    for layer in (1, 0):
        plan.restart(2)
        stages["down", layer] = plan.stage(range(0, 12, 2), 12, lambda t: t // 4 * 8 // 3)
        at = [4 * f + phase for f in range(8) for phase in ((0, 2, 3) if f in (0, 2) else (0, 2))]
        stages["hidden", layer] = plan.stage(at, PIECE, lambda j: j // 4 * 2 + j % 4 // 3)
        if layer:
            stages["states"] = plan.stage(range(16), 16, lambda j: 0)
    left = UNITS + LAST - plan.first
    first_left, low_left, _ = plan.stage(range(left), left, lambda j: 0)
    plan.check()

    def backward(i):
        layer, made = 1 - i, 24 * i

        def chosen(name):
            return tuple(jnp.where(i == 0, a, b) for a, b in zip(stages[name, 1], stages[name, 0]))

        def gradients(x2):
            take = pltpu.make_async_copy(a_all.at[layer], x2, load_sem.at[1])
            take.start()
            with jax.named_scope("down_gradient"):
                down_gradient(layer, made, chosen("down"))

            @pl.when(layer == 1)
            def _():
                def one(n):
                    gather.arrive(n, DOWN)

                loop(35, 38, one)

            take.wait()
            with jax.named_scope("hidden"):
                hidden(x2, layer, made + 8, chosen("hidden"))

        pl.run_scoped(gradients, pltpu.VMEM((M, D), BF))
        @pl.when(layer == 1)
        def _():
            with jax.named_scope("states"):
                states(stages["states"])


    pl.run_scoped(forward, pltpu.VMEM((M, D), BF))
    loop(0, 2, backward)

    def rest(t):
        scatter.tick(first_left + t, low_left, UNITS)

    with jax.named_scope("rest"):
        loop(0, left, rest)

    def last(u):
        scatter.write(u).wait()

    loop(UNITS - IN, UNITS, last)

    mine = jnp.sum(squares[:], axis=(0, 1), keepdims=True)
    sums[:] = jnp.broadcast_to(mine, sums.shape)

    def tell(to, of):
        return pltpu.make_async_remote_copy(
            src_ref=sums, dst_ref=sum_all.at[of], send_sem=sum_send.at[to], recv_sem=sum_recv.at[of], device_id={"dp": to}, device_id_type=MESH
        )

    for other in range(1, DEVICES):
        tell((me + other) % DEVICES, me).start()
    for other in range(1, DEVICES):
        tell((me + other) % DEVICES, (me + other) % DEVICES).wait_recv()
    for other in range(1, DEVICES):
        tell((me + other) % DEVICES, me).wait_send()
    sum_all[me] = sums[:]
    total = sum_all[0]
    for i in range(1, DEVICES):
        total = total + sum_all[i]
    total_ref[:] = total


def one_step(*args):
    any_spec = pl.BlockSpec(memory_space=pl.ANY)
    shape = jax.ShapeDtypeStruct
    piece = (COLORS, PIECE, BLOCK)
    dma = pltpu.SemaphoreType.DMA
    sums = [pltpu.VMEM((IN, COLORS, n, PIECE, BLOCK), BF) for n in (4, 2, 1)]
    outs = [
        shape((4, *SPREAD, FEW, F), BF), shape((LAYERS, *SPREAD, TALL, D), BF), shape((LAYERS, M, F), F32), shape((LAYERS, M, F), F32),
        shape((LAYERS, M, F), BF), shape((LAYERS, M, D), BF), shape((M, D), BF), shape((CORES, LAYERS, M, F), BF),
    ]
    outs = pl.pallas_call(
        step_kernel,
        out_shape=[*outs, shape((UNITS, FEW, BLOCK), BF), shape(TILE, F32)],
        in_specs=[any_spec] * 5,
        out_specs=[any_spec] * (len(outs) + 1) + [pl.BlockSpec(memory_space=pltpu.VMEM)],
        scratch_shapes=[
            pltpu.VMEM((M, D), BF),
            pltpu.VMEM((OWN, CORES, 8, *piece), BF),
            pltpu.VMEM((IN, 8, *piece), BF), *sums, *sums,
            pltpu.VMEM((IN, FEW, BLOCK), BF), pltpu.VMEM((8, BLOCK), F32), pltpu.VMEM(TILE, F32), pltpu.VMEM((DEVICES, *TILE), F32),
            dma((IN,)), dma((IN,)), *[dma((IN, COLORS))] * 6, dma((IN,)), pltpu.SemaphoreType.REGULAR((4,)),
            dma((DEVICES,)), dma((DEVICES,)), *[dma((9,))] * 3, *[dma((SLOTS, COLORS))] * 8,
        ],
        compiler_params=pltpu.CompilerParams(collective_id=0, has_side_effects=True, vmem_limit_bytes=VMEM),
        cost_estimate=pl.CostEstimate(flops=15 * 2 * M * D * F, bytes_accessed=900_000_000, transcendentals=0),
        name="training_step",
    )(*args)
    return outs[-2], outs[-1]


def adamw_kernel(total, *refs):
    count = LAYERS * COLORS * D * F
    factor = jnp.minimum(1.0, 0.5 * lax.rsqrt(total[:1, :1] / count + 1e-30))
    for i in range(COLORS):
        w, m, v, g, new_w, new_m, new_v = refs[i::COLORS]
        blocks = [(b, pl.ds(0, FEW), pl.ds(BLOCK * b, BLOCK)) for b in BOTH]
        if i == 2:
            blocks = [((c, r), pl.ds(PIECE * r, PIECE), pl.ds(BLOCK * c, BLOCK)) for c in range(COLORS) for r in BOTH]
        for at, rows, columns in blocks:
            by = (g[0, at, 0] if i < 2 else g[0, at[0], at[1]]).astype(F32) * factor
            new_w[0, rows, columns], new_m[0, rows, columns], new_v[0, rows, columns] = adamw(
                w[0, rows, columns].astype(F32), m[0, rows, columns], v[0, rows, columns], by
            )


def optimizer(total, weights, m, v, units):
    wide = pl.BlockSpec((1, FEW, WIDTH), lambda layer, i: (layer, 0, i))
    down = pl.BlockSpec((1, ROWS, D), lambda layer, i: (layer, i, 0))
    blocks = [wide, wide, down]

    def order(which):
        return lambda layer, i: (1 - layer, 2 + i, which, 0, 0)

    gradients = [pl.BlockSpec((1, 2, 1, FEW, BLOCK), order(0)), pl.BlockSpec((1, 2, 1, FEW, BLOCK), order(1))]
    gradients.append(pl.BlockSpec((1, 3, 2, PIECE, BLOCK), lambda layer, i: (1 - layer, 0, i, 0, 0)))
    by_columns, by_rows = units.reshape(2, 12, 2, FEW, BLOCK), units.reshape(2, 9, 8, PIECE, BLOCK)
    return pl.pallas_call(
        adamw_kernel,
        grid=(2, 4),
        out_shape=[jax.ShapeDtypeStruct(w.shape, BF) for w in weights] + [jax.ShapeDtypeStruct(a.shape, F32) for a in (*m, *v)],
        in_specs=[pl.BlockSpec(TILE, lambda layer, i: (0, 0)), *blocks * 3, *gradients],
        out_specs=blocks * 3,
        compiler_params=pltpu.CompilerParams(vmem_limit_bytes=VMEM),
        name="optimizer",
    )(total, *weights, *m, *v, by_columns, by_columns, by_rows)


def solution(mesh):
    def step(x, dy, *arrays):
        weights, m, v = (arrays[i : i + 3] for i in (0, 3, 6))
        units, total = one_step(x[0], dy[0], *weights)
        return tuple(optimizer(total, weights, m, v, units))

    states, cut = P(("rep", "dp"), None, None), P(None, "dp", None)
    return jax.shard_map(
        step,
        mesh=mesh,
        in_specs=(states, states) + (cut,) * 9,
        out_specs=(P("rep", "dp", None),) * 9,
        check_vma=False,
    )
```
